128 devices in a mesh: row: 8 (over y_hi, z), col: 16 (over x, y_lo, core).
Axes of the slice: x: 4, y: 4 (y_hi: 2, y_lo: 2; y = y_hi * 2 + y_lo), z: 4, core: 2. Of those that a mesh axis runs over, the one named last changes fastest.
Arguments:
- activations: bfloat16 [8192, 8192], P('col', 'row'), may hold values from -6 to 6
- out_grads: bfloat16 [8192, 4096], P('row', 'col'), may hold values from -0.0625 to 0.0625
- statistics: float32 [8, 16, 512, 1024], P('row', 'col'), may hold values from -10 to 200, as said below
Outputs:
- new_statistics: float32 [8, 16, 512, 1024], P('row', 'col')
- update: bfloat16 [8192, 4096], P('row', 'col')
The draws below stay inside these ranges and needn't reach their ends.
Inputs may be any that keep to these rules, and one draw needn't show every extreme that they name: `statistics`: every statistic is symmetric and positive definite.
All inputs are finite; a program needn't handle non-finite values.
Results may differ from the reference program's by a relative error of at most 0.0017.
The reference program's roundings to bfloat16 on the way count: a program that leaves them out, or rounds other values in their place, can miss the bound.
Values may be sent and summed in bfloat16 or wider, within the bound.
No kernel may reach another device: no remote copies, remote signals or barrier semaphores. Data moves between devices by JAX's collectives and lax.ppermute only.
A program may use at most 128 MiB of HBM per device.

```python
import math
import jax
import jax.numpy as jnp
from jax import lax

BLOCK = 1024
ITERS = 2
DAMP_EXP = 3
TOKENS = 8192
D_IN = 8192
D_OUT = 4096


def draw_statistics(key, part):
    in_count = D_IN // BLOCK
    out_count = D_OUT // BLOCK
    stat_count = in_count * out_count * 2
    noise_key, diagonal_key, scale_key = jax.random.split(jax.random.fold_in(key, 17), 3)
    noise_draw = jax.random.normal(noise_key, (stat_count, BLOCK, BLOCK), jnp.float32)
    symmetric = (noise_draw + jnp.swapaxes(noise_draw, 1, 2)) * (0.70710678 / 80.0)
    diagonal = jax.random.uniform(diagonal_key, (stat_count, BLOCK), jnp.float32, 1.0, 2.0)
    upper_scale = 3.0
    scales = jnp.exp(jax.random.uniform(scale_key, (stat_count, BLOCK), jnp.float32, 0.0, math.log(upper_scale)))
    identity = jnp.eye(BLOCK, dtype=jnp.float32)
    base_matrix = symmetric * (1.0 - identity)[None] + identity[None] * diagonal[:, :, None]
    full_stats = scales[:, :, None] * base_matrix * scales[:, None, :]
    full_stats = full_stats.reshape(in_count, out_count, 2, 2, BLOCK // 2, BLOCK).transpose(0, 1, 3, 2, 4, 5)
    return full_stats.reshape(in_count, 4 * out_count, BLOCK // 2, BLOCK)


def block_scale(key, dims, cuts, low, high):
    gain, own = 1.0, jax.random.fold_in(key, 6)
    for dim, blocks in cuts:
        steps = jnp.exp(jax.random.uniform(jax.random.fold_in(own, dim), (blocks,), jnp.float32, low / len(cuts), high / len(cuts)))
        gain = gain * jnp.repeat(steps, dims[dim] // blocks).reshape([-1 if axis == dim else 1 for axis in range(len(dims))])
    return gain


def normal_values(rng, shape, scale, most, cuts=(), kind=jnp.bfloat16):
    values = scale * jax.random.normal(rng, shape, jnp.float32)
    if cuts:
        values = values * block_scale(rng, shape, cuts, -0.22, 0.18)
    return jnp.clip(values, -most, most).astype(kind)


def setup_inputs(seed: int = 0) -> dict:
    key_list = jax.random.split(jax.random.key(seed), 4)
    activations = normal_values(key_list[0], (TOKENS, D_IN), 1.0, 6.0, ((0, 16), (1, 8)))
    out_grads = normal_values(key_list[1], (TOKENS, D_OUT), TOKENS ** -0.5, 0.0625, ((0, 8), (1, 16)))
    statistics = draw_statistics(jax.random.fold_in(key_list[3], 71), 0)
    return dict(activations=activations, out_grads=out_grads, statistics=statistics)


DECAY = 0.9
EPS = 1e-06

def matmul_high(left, right):
    return jnp.dot(left, right, precision=lax.Precision.HIGHEST, preferred_element_type=jnp.float32)

def inverse_root(statistic):
    matrix_order = statistic.shape[0]
    identity = jnp.eye(matrix_order, dtype=jnp.float32)
    damping = 10.0 ** (-DAMP_EXP) * jnp.trace(statistic) / matrix_order
    damped = statistic + damping * identity
    scaling = jnp.max(lax.optimization_barrier(jnp.sum(jnp.abs(damped), axis=1))) / 4.0
    normed = damped / scaling
    result = identity
    for iteration in range(ITERS):
        factor = (5.0 * identity - normed) / 4.0
        if iteration == 0:
            result = factor
        else:
            result = matmul_high(result, factor)
        if iteration + 1 < ITERS:
            square = matmul_high(factor, factor)
            fourth = matmul_high(square, square)
            normed = matmul_high(fourth, normed)
    return result

def one_block(block_item):
    grad_block, old_pair = block_item
    left_gram = jnp.dot(grad_block, grad_block.T, preferred_element_type=jnp.float32)
    right_gram = jnp.dot(grad_block.T, grad_block, preferred_element_type=jnp.float32)
    renewed = jnp.stack([DECAY * old_pair[0] + (1.0 - DECAY) / BLOCK * left_gram, DECAY * old_pair[1] + (1.0 - DECAY) / BLOCK * right_gram])
    left_root = inverse_root(old_pair[0]).astype(jnp.bfloat16)
    right_root = inverse_root(old_pair[1]).astype(jnp.bfloat16)
    half_product = jnp.dot(grad_block, right_root, preferred_element_type=jnp.float32).astype(jnp.bfloat16)
    conditioned = jnp.dot(left_root, half_product, preferred_element_type=jnp.float32)
    column_tiles = conditioned.reshape(BLOCK, 4, BLOCK // 4)
    grad_tiles = grad_block.astype(jnp.float32).reshape(BLOCK, 4, BLOCK // 4)
    grad_power = lax.optimization_barrier(jnp.mean(grad_tiles * grad_tiles, axis=(0, 2)))
    cond_power = lax.optimization_barrier(jnp.mean(column_tiles * column_tiles, axis=(0, 2)))
    graft_ratio = jnp.sqrt(grad_power / (cond_power + EPS))
    update = (column_tiles * graft_ratio[None, :, None]).reshape(BLOCK, BLOCK).astype(jnp.bfloat16)
    return (renewed, update)

def reference(activations, out_grads, statistics):
    gradient = jnp.dot(activations.T, out_grads, preferred_element_type=jnp.float32).astype(jnp.bfloat16)
    in_count = D_IN // BLOCK
    out_count = D_OUT // BLOCK
    grad_blocks = gradient.reshape(in_count, BLOCK, out_count, BLOCK).transpose(0, 2, 1, 3).reshape(-1, BLOCK, BLOCK)
    previous = statistics.reshape(in_count, out_count, 2, 2, BLOCK // 2, BLOCK).transpose(0, 1, 3, 2, 4, 5)
    previous = previous.reshape(in_count * out_count, 2, BLOCK, BLOCK)
    renewed, updates = lax.map(one_block, (grad_blocks, previous))
    new_statistics = renewed.reshape(in_count, out_count, 2, 2, BLOCK // 2, BLOCK).transpose(0, 1, 3, 2, 4, 5)
    new_statistics = new_statistics.reshape(in_count, 4 * out_count, BLOCK // 2, BLOCK)
    update = updates.reshape(in_count, out_count, BLOCK, BLOCK).transpose(0, 2, 1, 3).reshape(D_IN, D_OUT)
    return (new_statistics, update)
```

```python
import jax
import jax.numpy as jnp
from jax import lax
from jax.experimental import pallas as pl
from jax.experimental.pallas import tpu as pltpu
from jax.sharding import Mesh
from jax.sharding import PartitionSpec as P


DAMP = 10.0 ** (-3)
DECAY = 0.9
EPS = 1e-06
F32 = jnp.float32
BF16 = jnp.bfloat16
TILE = 256


VMEM = pl.BlockSpec(memory_space=pltpu.VMEM)
SMEM = pl.BlockSpec(memory_space=pltpu.SMEM)


def shift(value, axis, step):
    count = lax.axis_size(axis)
    return lax.ppermute(value, axis, [(k, (k + step) % count) for k in range(count)])


def aligned(start, size):
    return pl.ds(pl.multiple_of(start, size), size)


def split(value):
    high = value.astype(BF16)
    return high, (value - high.astype(F32)).astype(BF16)


def put_left(left, rows, cols, value):
    n = left.shape[0]
    high, low = split(value)
    left[rows, cols] = high
    left[rows, n + cols.start : n + cols.stop] = high
    left[rows, 2 * n + cols.start : 2 * n + cols.stop] = low


def put_right(right, rows, cols, value):
    n = right.shape[1]
    high, low = split(value)
    right[rows, cols] = high
    right[n + rows.start : n + rows.stop, cols] = low
    right[2 * n + rows.start : 2 * n + rows.stop, cols] = high


def put_symmetric(put, target, j, upper):
    start = j * TILE
    cols = slice(start, start + TILE)
    put(target, slice(0, start + TILE), cols, upper)
    for i in range(j):
        part = slice(i * TILE, (i + 1) * TILE)
        put(target, cols, part, upper[part, :].T)


def symmetric_product(left, right, emit):
    for j in range(right.shape[1] // TILE):
        start = j * TILE
        upper = jnp.dot(
            left[: start + TILE, :], right[:, start : start + TILE], preferred_element_type=F32
        )
        emit(j, upper)


def square_kernel(where, own, other, factor, square, stat, left, right):
    n = stat.shape[0]
    half = n // 2
    h = where[0]
    mine, his = aligned(h * half, half), aligned((1 - h) * half, half)
    quarter = half // 2
    first, second = aligned((1 - h) * half, quarter), aligned((1 - h) * half + quarter, quarter)
    stat[mine, :] = own[...]
    stat[first, his] = other[:, :half]
    stat[second, first] = other[:, quarter:half].T
    stat[second, second] = other[:, half:]
    stat[his, mine] = own[:, his].T

    row = lax.broadcasted_iota(jnp.int32, (TILE, TILE), 0)
    eye = row == lax.broadcasted_iota(jnp.int32, (TILE, TILE), 1)

    def sums(k, carry):
        trace, most = carry
        cols = aligned(k * TILE, TILE)
        trace += jnp.sum(jnp.where(eye, stat[cols, cols], 0.0))
        return trace, jnp.maximum(most, jnp.max(jnp.sum(jnp.abs(stat[:, cols]), axis=0)))

    trace, most = lax.fori_loop(0, n // TILE, sums, (F32(0.0), F32(0.0)))
    damping = DAMP * trace / n
    inverse = 1.0 / (most + damping)
    for i in range(n // TILE):
        rows = slice(i * TILE, (i + 1) * TILE)
        for j in range(n // TILE):
            cols = slice(j * TILE, (j + 1) * TILE)
            value = -stat[rows, cols] * inverse
            if i == j:
                value = jnp.where(eye, (1.25 - damping * inverse) + value, value)
            factor[rows, cols] = value
            put_left(left, rows, cols, value)
            put_right(right, rows, cols, value)

    def squared(j, upper):
        end = (j + 1) * TILE
        square[:end, j * TILE : end] = upper

    symmetric_product(left, right, squared)


def root_kernel(factor, square, root, left, right, left2, right2):
    for j in range(factor.shape[0] // TILE):
        end = (j + 1) * TILE
        upper = square[:end, j * TILE : end]
        put_symmetric(put_left, left2, j, upper)
        put_symmetric(put_right, right2, j, upper)

    def fourth(j, upper):
        end = (j + 1) * TILE
        cols = slice(j * TILE, end)
        put_symmetric(put_left, left, j, upper)
        put_symmetric(put_right, right, j, 5.0 * factor[:end, cols] - 4.0 * square[:end, cols])

    symmetric_product(left2, right2, fourth)

    def last(j, upper):
        end = (j + 1) * TILE
        cols = slice(j * TILE, end)
        value = 1.25 * factor[:end, cols] - 0.25 * upper
        root[:end, cols] = value.astype(BF16)
        for i in range(j):
            part = slice(i * TILE, (i + 1) * TILE)
            root[cols, part] = value[part, :].T.astype(BF16)

    symmetric_product(left, right, last)


def transposed(piece, grads):
    return lax.dot_general(
        piece, grads, (((0,), (0,)), ((), ())), preferred_element_type=F32
    )


def first_kernel(slot, *refs):
    own, far, partner, grads = refs[:3], refs[3:5], refs[5:9], refs[9:17]
    total, second, right = refs[17:]
    for k in range(8):
        right[slot[k]] = grads[k][...]
    rows = total.shape[0]
    cut = right.shape[1] // 2
    for part, out in ((slice(0, rows), total), (slice(rows, 2 * rows), second)):
        value = transposed(own[0][:, part], right[0])
        value += transposed(own[1][:, part], right[1])
        value += transposed(own[2][:, part], right[3])
        value += transposed(far[0][:, part], right[2, :cut, :])
        value += transposed(far[1][:, part], right[2, cut:, :])
        if out is total:
            for k in range(4):
                value += transposed(partner[k][...], right[4 + k])
        out[...] = value


def second_kernel(*refs):
    partner, (right, second, total) = refs[:4], refs[4:]
    value = second[...]
    for k in range(4):
        value += transposed(partner[k][...], right[4 + k])
    total[...] = value


def final_kernel(where, own, mine, other, *refs):
    tiles, (renewed, update, block, cond) = refs[:8], refs[8:]
    n = block.shape[0]
    width = tiles[0].shape[1]
    half = n // 2
    h, s = where[0], where[1]
    for dh in range(2):
        for ds in range(2):
            cols = aligned((2 * (h + dh - 2 * h * dh) + (s + ds - 2 * s * ds)) * width, width)
            block[:half, cols] = tiles[2 * dh + ds][...]
            block[half:, cols] = tiles[4 + 2 * dh + ds][...]
    rows = aligned(h * half, half)
    tile = aligned((2 * h + s) * width, width)

    def renew(gram):
        renewed[...] = DECAY * own[...] + ((1.0 - DECAY) / n) * gram

    def condition(left, right):
        product = jnp.dot(block[...], right[:, tile], preferred_element_type=F32).astype(BF16)
        cond[...] = jnp.dot(left[...], product, preferred_element_type=F32)

    @pl.when(s == 0)
    def _():
        renew(lax.dot_general(
            block[rows, :], block[...], (((1,), (1,)), ((), ())), preferred_element_type=F32))
        condition(mine, other)

    @pl.when(s == 1)
    def _():
        renew(lax.dot_general(
            block[:, rows], block[...], (((0,), (0,)), ((), ())), preferred_element_type=F32))
        condition(other, mine)

    values = block[:, tile].astype(F32)
    conditioned = cond[...]
    count = n * width
    power = jnp.sum(values * values) / count
    base = jnp.sum(conditioned * conditioned) / count + EPS
    update[...] = (conditioned * jnp.sqrt(power / base)).astype(BF16)


def resident(value):
    return pltpu.with_memory_space_constraint(value, pltpu.VMEM)


def call(kernel, out, args, in_specs, out_specs, scratch, flops, limit):
    return pl.pallas_call(
        kernel,
        out_shape=out,
        in_specs=in_specs,
        out_specs=out_specs,
        scratch_shapes=scratch,
        cost_estimate=pl.CostEstimate(flops=flops, transcendentals=0, bytes_accessed=2**23),
        compiler_params=pltpu.CompilerParams(vmem_limit_bytes=limit * 2**20),
    )(*[arg if spec is SMEM else resident(arg) for arg, spec in zip(args, in_specs)])


def root_of(where, own, other):
    n = own.shape[1]
    wide = pltpu.VMEM((n, n), F32)
    pair = [pltpu.VMEM((n, 3 * n), BF16), pltpu.VMEM((3 * n, n), BF16)]
    factor, square = call(
        square_kernel, (wide, wide), (where, own, other),
        [SMEM, VMEM, VMEM], (VMEM, VMEM), [wide] + pair, 4 * n**3, 20,
    )
    return call(
        root_kernel, pltpu.VMEM((n, n), BF16), (factor, square),
        [VMEM, VMEM], VMEM, pair + pair, 8 * n**3, 28,
    )


def first_gradient(slot, own, far, partner, grads):
    tokens, width = grads[0].shape
    rows = own[0].shape[1] // 2
    part = pltpu.VMEM((rows, width), F32)
    return call(
        first_kernel, (part, part, pltpu.VMEM((8, tokens, width), BF16)),
        (slot, *own, *far, *partner, *grads), [SMEM] + [VMEM] * 17, (VMEM,) * 3, [],
        24 * tokens * rows * width, 14,
    )


def second_gradient(partner, right, second):
    rows, width = second.shape
    return call(
        second_kernel, pltpu.VMEM((rows, width), F32), (*partner, right, second),
        [VMEM] * 6, VMEM, [], 8 * right.shape[1] * rows * width, 10,
    )


def finish(where, own, mine, other, tiles):
    n = mine.shape[0]
    half, width = n // 2, tiles[0].shape[1]
    scratch = [pltpu.VMEM((n, n), BF16), pltpu.VMEM((n, width), F32)]
    out = (jax.ShapeDtypeStruct((half, n), F32), jax.ShapeDtypeStruct((n, width), BF16))
    return call(
        final_kernel, out, (where, own, mine, other, *tiles),
        [SMEM] + [VMEM] * (3 + len(tiles)), (VMEM, VMEM), scratch, 4 * n**3, 14,
    )


def step(activations, out_grads, statistics):
    own = statistics[0, 0]
    half, _ = own.shape
    width = out_grads.shape[1]
    x, z, yh = lax.axis_index("x"), lax.axis_index("z"), lax.axis_index("yh")
    h, s = lax.axis_index("yl"), lax.axis_index("core")
    where = jnp.stack([h, s]).astype(jnp.int32)

    cut = activations.shape[0] // 2
    below, above = shift(activations, "x", 1), shift(activations, "x", -1)
    mine = [activations, above, below]
    far = [shift(below[:cut], "x", 1), shift(above[cut:], "x", -1)]
    partner = []
    for m in range(2):
        across = shift(activations[:, m * half : (m + 1) * half], "yl", 1)
        below, above = shift(across, "x", 1), shift(across, "x", -1)
        last = shift(below, "x", 1) if m == 0 else shift(above, "x", -1)
        partner.append([across, above, last, below])

    tokens = out_grads.shape[0] // 2
    keep = lax.dynamic_slice_in_dim(out_grads, s * tokens, tokens, 0)
    give = lax.dynamic_slice_in_dim(out_grads, (1 - s) * tokens, tokens, 0)
    pair = jnp.concatenate([keep, shift(give, "core", 1)], 1)
    across = shift(pair, "yh", 1)
    below, above = shift(pair, "z", 1), shift(pair, "z", -1)
    grads = [pair, above, shift(below, "z", 1), below]
    below, above = shift(across, "z", 1), shift(across, "z", -1)
    grads += [across, above, shift(above, "z", -1), below]
    slot = []
    for dy in range(2):
        for dz in range(4):
            chunk = 4 * ((yh + dy) % 2) + (z + dz) % 4
            slot.append(4 * ((chunk + h) % 2) + (chunk // 2 - x) % 4)
    slot = jnp.stack(slot).astype(jnp.int32)

    quadrant = lax.dynamic_slice_in_dim(own, h * half, half, 1)
    packed = jnp.concatenate([quadrant[: half // 2], quadrant[half // 2 :, half // 2 :]], 1)
    root = root_of(where, own, shift(packed, "yl", 1))
    other = shift(root, "core", 1)

    total, second, right = first_gradient(slot, mine, far, partner[0], grads)
    tiles = []
    for m in range(2):
        if m == 1:
            total = second_gradient(partner[1], right, second)
        given = shift(total, "core", 1)
        tile = (total[:, :width] + given[:, width:]).astype(BF16)
        beside = (total[:, width:] + given[:, :width]).astype(BF16)
        across = shift(tile, "yl", 1)
        tiles += [tile, beside, across, shift(across, "core", 1)]

    renewed, update = finish(where, own, root, other, tiles)
    return renewed[None, None], update


def solution(mesh):
    torus = Mesh(mesh.devices.reshape(2, 4, 4, 2, 2), ("yh", "z", "x", "yl", "core"))
    row, col = ("yh", "z"), ("x", "yl", "core")
    return jax.shard_map(
        step,
        mesh=torus,
        in_specs=(P(col, row), P(row, col), P(row, col, None, None)),
        out_specs=(P(row, col, None, None), P(row, col)),
        check_vma=False,
    )
```

```python
import jax
import jax.numpy as jnp
from jax import lax
from jax.experimental import pallas as pl
from jax.experimental.pallas import tpu as pltpu
from jax.sharding import Mesh
from jax.sharding import PartitionSpec as P


DAMP = 10.0 ** (-3)
DECAY = 0.9
EPS = 1e-06
F32 = jnp.float32
BF16 = jnp.bfloat16
TILE = 256
SIZES = (512, 512)


VMEM = pl.BlockSpec(memory_space=pltpu.VMEM)
SMEM = pl.BlockSpec(memory_space=pltpu.SMEM)


def shift(value, axis, step):
    count = lax.axis_size(axis)
    return lax.ppermute(value, axis, [(k, (k + step) % count) for k in range(count)])


def aligned(start, size):
    return pl.ds(pl.multiple_of(start, size), size)


def split(value):
    high = value.astype(BF16)
    return high, (value - high.astype(F32)).astype(BF16)


def put_left(left, rows, cols, value):
    n = left.shape[0]
    high, low = split(value)
    left[rows, cols] = high
    left[rows, n + cols.start : n + cols.stop] = high
    left[rows, 2 * n + cols.start : 2 * n + cols.stop] = low


def put_right(right, rows, cols, value):
    n = right.shape[1]
    high, low = split(value)
    right[rows, cols] = high
    right[n + rows.start : n + rows.stop, cols] = low
    right[2 * n + rows.start : 2 * n + rows.stop, cols] = high


def put_symmetric(put, target, j, upper):
    start = j * TILE
    cols = slice(start, start + TILE)
    put(target, slice(0, start + TILE), cols, upper)
    for i in range(j):
        part = slice(i * TILE, (i + 1) * TILE)
        put(target, cols, part, upper[part, :].T)


def symmetric_product(left, right, emit):
    for j in range(right.shape[1] // TILE):
        start = j * TILE
        upper = jnp.dot(
            left[: start + TILE, :], right[:, start : start + TILE], preferred_element_type=F32
        )
        emit(j, upper)


def square_kernel(where, own, other, factor, square, stat, left, right):
    n = stat.shape[0]
    half = n // 2
    h = where[0]
    mine, his = aligned(h * half, half), aligned((1 - h) * half, half)
    stat[mine, :] = own[...]
    step, start, width = other.shape[0], 0, half
    for k in range(half // other.shape[0]):
        rows = aligned((1 - h) * half + k * step, step)
        stat[rows, aligned((1 - h) * half + k * step, step)] = other[:, start : start + step]
        for j in range(1, width // step):
            cols = aligned((1 - h) * half + (k + j) * step, step)
            block = other[:, start + j * step : start + (j + 1) * step]
            stat[rows, cols] = block
            stat[cols, rows] = block.T
        start, width = start + width, width - step
    stat[his, mine] = own[:, his].T

    row = lax.broadcasted_iota(jnp.int32, (TILE, TILE), 0)
    eye = row == lax.broadcasted_iota(jnp.int32, (TILE, TILE), 1)

    def sums(k, carry):
        trace, most = carry
        cols = aligned(k * TILE, TILE)
        trace += jnp.sum(jnp.where(eye, stat[cols, cols], 0.0))
        return trace, jnp.maximum(most, jnp.max(jnp.sum(jnp.abs(stat[:, cols]), axis=0)))

    trace, most = lax.fori_loop(0, n // TILE, sums, (F32(0.0), F32(0.0)))
    damping = DAMP * trace / n
    inverse = 1.0 / (most + damping)
    for i in range(n // TILE):
        rows = slice(i * TILE, (i + 1) * TILE)
        for j in range(n // TILE):
            cols = slice(j * TILE, (j + 1) * TILE)
            value = -stat[rows, cols] * inverse
            if i == j:
                value = jnp.where(eye, (1.25 - damping * inverse) + value, value)
            factor[rows, cols] = value
            put_left(left, rows, cols, value)
            put_right(right, rows, cols, value)

    def squared(j, upper):
        end = (j + 1) * TILE
        square[:end, j * TILE : end] = upper

    symmetric_product(left, right, squared)


def root_kernel(factor, square, root, left, right, left2, right2):
    for j in range(factor.shape[0] // TILE):
        end = (j + 1) * TILE
        upper = square[:end, j * TILE : end]
        put_symmetric(put_left, left2, j, upper)
        put_symmetric(put_right, right2, j, upper)

    def fourth(j, upper):
        end = (j + 1) * TILE
        cols = slice(j * TILE, end)
        put_symmetric(put_left, left, j, upper)
        put_symmetric(put_right, right, j, 5.0 * factor[:end, cols] - 4.0 * square[:end, cols])

    symmetric_product(left2, right2, fourth)

    def last(j, upper):
        end = (j + 1) * TILE
        cols = slice(j * TILE, end)
        value = 1.25 * factor[:end, cols] - 0.25 * upper
        root[:end, cols] = value.astype(BF16)
        for i in range(j):
            part = slice(i * TILE, (i + 1) * TILE)
            root[cols, part] = value[part, :].T.astype(BF16)

    symmetric_product(left, right, last)


def times(left, right):
    return jnp.dot(left, right, preferred_element_type=F32)


LAST = 6


def add_own(total, j, own, grads, part):
    half = grads.shape[1] // 2
    if j == 2:
        total[:, part] += times(grads[:, :half], own[3][...]) + times(grads[:, half:], own[4][...])
    else:
        total[:, part] += times(grads, own[(0, 1, 3, 2)[j]][...])


def own_kernel(slot, *refs):
    own, grads, (total, right, stack) = refs[:5], refs[5:12], refs[12:]
    tokens, width = right.shape[2], right.shape[1] // 2
    for k, piece in zip([k for k in range(8) if k != LAST], grads):
        stack[slot[k], :width, :] = piece[:tokens, :].T
        stack[slot[k], width:, :] = piece[tokens:, :].T
    right[...] = stack[4:]
    total[...] = jnp.zeros(total.shape, F32)
    for j in range(4):
        @pl.when(slot[LAST] != j)
        def _(j=j):
            add_own(total, j, own, stack[j], slice(None))


def partner_kernel(m):
    start = sum(SIZES[:m])

    def add(slot, own, pieces, right, before, late, total):
        value = before[:, start : start + total.shape[1]]
        for k in range(4):
            value += times(right[k], pieces[k][...])
        total[...] = value
        part = pl.ds(start, total.shape[1])
        views = [piece.at[:, part] for piece in own]
        for j in range(4):
            @pl.when(slot[LAST] == j)
            def _(j=j):
                add_own(total, j, views, late[...], slice(None))

    def first(slot, *refs):
        own, pieces, (last, right, before, total, full, late) = refs[:5], refs[5:9], refs[9:]
        tokens, width = right.shape[2], right.shape[1] // 2
        late[:width, :] = last[:tokens, :].T
        late[width:, :] = last[tokens:, :].T
        full[...] = right[...]

        @pl.when(slot[LAST] >= 4)
        def _():
            full[jnp.maximum(slot[LAST] - 4, 0)] = late[...]

        add(slot, own, pieces, full, before, late, total)

    def second(slot, *refs):
        own, pieces, (right, before, late, total) = refs[:5], refs[5:9], refs[9:]
        add(slot, own, pieces, right, before, late, total)

    return second if m else first


def gram_kernel(where, own, *refs):
    tiles, (renewed, block) = refs[:8], refs[8:]
    n = block.shape[0]
    width = tiles[0].shape[0]
    half = n // 2
    h, s = where[0], where[1]
    for dh in range(2):
        for ds in range(2):
            cols = aligned((2 * (h + dh - 2 * h * dh) + (s + ds - 2 * s * ds)) * width, width)
            block[cols, : SIZES[0]] = tiles[2 * dh + ds][...]
            block[cols, SIZES[0] :] = tiles[4 + 2 * dh + ds][...]
    rows = aligned(h * half, half)

    def renew(gram):
        renewed[...] = DECAY * own[...] + ((1.0 - DECAY) / n) * gram

    @pl.when(s == 0)
    def _():
        renew(lax.dot_general(
            block[:, rows], block[...], (((0,), (0,)), ((), ())), preferred_element_type=F32))

    @pl.when(s == 1)
    def _():
        renew(lax.dot_general(
            block[rows, :], block[...], (((1,), (1,)), ((), ())), preferred_element_type=F32))


def update_kernel(where, block, mine, other, update, cond):
    n, width = update.shape
    h, s = where[0], where[1]
    tile = aligned((2 * h + s) * width, width)

    def condition(left, right):
        product = times(right[tile, :], block[...]).astype(BF16)
        cond[...] = times(product, left[...])

    @pl.when(s == 0)
    def _():
        condition(mine, other)

    @pl.when(s == 1)
    def _():
        condition(other, mine)

    values = block[tile, :].astype(F32)
    conditioned = cond[...]
    count = n * width
    power = jnp.sum(values * values) / count
    base = jnp.sum(conditioned * conditioned) / count + EPS
    update[...] = (conditioned * jnp.sqrt(power / base)).astype(BF16).T


def resident(value):
    return pltpu.with_memory_space_constraint(value, pltpu.VMEM)


def call(kernel, out, args, in_specs, out_specs, scratch, flops, limit):
    return pl.pallas_call(
        kernel,
        out_shape=out,
        in_specs=in_specs,
        out_specs=out_specs,
        scratch_shapes=scratch,
        cost_estimate=pl.CostEstimate(flops=flops, transcendentals=0, bytes_accessed=2**23),
        compiler_params=pltpu.CompilerParams(vmem_limit_bytes=limit * 2**20),
    )(*[arg if spec is SMEM else resident(arg) for arg, spec in zip(args, in_specs)])


def root_of(where, own, other):
    n = own.shape[1]
    wide = pltpu.VMEM((n, n), F32)
    pair = [pltpu.VMEM((n, 3 * n), BF16), pltpu.VMEM((3 * n, n), BF16)]
    factor, square = call(
        square_kernel, (wide, wide), (where, own, other),
        [SMEM, VMEM, VMEM], (VMEM, VMEM), [wide] + pair, 4 * n**3, 20,
    )
    return call(
        root_kernel, pltpu.VMEM((n, n), BF16), (factor, square),
        [VMEM, VMEM], VMEM, pair + pair, 8 * n**3, 28,
    )


def own_gradient(slot, own, grads):
    tokens, rows = own[0].shape
    width = 2 * grads[0].shape[1]
    return call(
        own_kernel,
        (pltpu.VMEM((width, rows), F32), pltpu.VMEM((4, width, tokens), BF16)),
        (slot, *own, *grads), [SMEM] + [VMEM] * 12, (VMEM, VMEM),
        [pltpu.VMEM((8, width, tokens), BF16)], 8 * tokens * rows * width, 14,
    )


def whole_gradient(m, slot, own, partner, right, before, last):
    width, tokens = right.shape[1:]
    out = [pltpu.VMEM((width, SIZES[m]), F32)]
    args = (slot, *own, *partner, right, before, last)
    if m == 0:
        out += [pltpu.VMEM(right.shape, BF16), pltpu.VMEM((width, tokens), BF16)]
        args = (slot, *own, *partner, last, right, before)
    return call(
        partner_kernel(m), tuple(out), args, [SMEM] + [VMEM] * 12,
        (VMEM,) * len(out), [], 8 * tokens * SIZES[m] * width, 10,
    )


def finish(where, own, mine, other, tiles):
    n = mine.shape[0]
    half, width = n // 2, tiles[0].shape[0]
    renewed, block = call(
        gram_kernel, (jax.ShapeDtypeStruct((half, n), F32), pltpu.VMEM((n, n), BF16)),
        (where, own, *tiles), [SMEM] + [VMEM] * (1 + len(tiles)), (VMEM, VMEM), [], 2 * n**3, 12,
    )
    update = call(
        update_kernel, jax.ShapeDtypeStruct((n, width), BF16),
        (where, block, mine, other), [SMEM] + [VMEM] * 3, VMEM, [pltpu.VMEM((width, n), F32)],
        2 * n**3, 12,
    )
    return renewed, update


def step(activations, out_grads, statistics):
    own = statistics[0, 0]
    half, _ = own.shape
    width = out_grads.shape[1]
    x, z, yh = lax.axis_index("x"), lax.axis_index("z"), lax.axis_index("yh")
    h, s = lax.axis_index("yl"), lax.axis_index("core")
    where = jnp.stack([h, s]).astype(jnp.int32)

    cut = activations.shape[0] // 2
    below, above = shift(activations, "x", 1), shift(activations, "x", -1)
    far = [shift(below[:cut], "x", 1), shift(above[cut:], "x", -1)]
    mine = [activations, above, below] + far
    partner = []
    for m, size in enumerate(SIZES):
        start = sum(SIZES[:m])
        source = lax.optimization_barrier((activations, out_grads))[0] if m else activations
        across = shift(source[:, start : start + size], "yl", 1)
        below, above = shift(across, "x", 1), shift(across, "x", -1)
        last = shift(below, "x", 1) if m == 0 else shift(above, "x", -1)
        partner.append([across, above, last, below])

    tokens = out_grads.shape[0] // 2
    keep = lax.dynamic_slice_in_dim(out_grads, s * tokens, tokens, 0)
    give = lax.dynamic_slice_in_dim(out_grads, (1 - s) * tokens, tokens, 0)
    pair = jnp.concatenate([keep, shift(give, "core", 1)], 0)
    across = shift(pair, "yh", 1)
    below, above = shift(pair, "z", 1), shift(pair, "z", -1)
    grads = [pair, above, shift(below, "z", 1), below]
    below, above = shift(across, "z", 1), shift(across, "z", -1)
    grads += [across, above, shift(above, "z", -1), below]
    slot = []
    for dy in range(2):
        for dz in range(4):
            chunk = 4 * ((yh + dy) % 2) + (z + dz) % 4
            slot.append(4 * ((chunk + h) % 2) + (chunk // 2 - x) % 4)
    slot = jnp.stack(slot).astype(jnp.int32)

    quadrant = lax.dynamic_slice_in_dim(own, h * half, half, 1)
    cut = half // 4
    packed = [quadrant[k : k + cut, k:] for k in range(0, half, cut)]
    packed = jnp.concatenate(packed, 1)
    root = root_of(where, own, shift(packed, "yl", 1))
    other = shift(root, "core", 1)

    last = grads.pop(LAST)
    part, right = own_gradient(slot, mine, grads)
    tiles = []
    for m in range(2):
        if m == 0:
            total, right, last = whole_gradient(m, slot, mine, partner[m], right, part, last)
        else:
            (total,) = whole_gradient(m, slot, mine, partner[m], right, part, last)
        given = shift(total, "core", 1)
        tile = (total[:width] + given[width:]).astype(BF16)
        beside = (total[width:] + given[:width]).astype(BF16)
        across = shift(tile, "yl", 1)
        tiles += [tile, beside, across, shift(across, "core", 1)]

    renewed, update = finish(where, own, root, other, tiles)
    return renewed[None, None], update


def solution(mesh):
    torus = Mesh(mesh.devices.reshape(2, 4, 4, 2, 2), ("yh", "z", "x", "yl", "core"))
    row, col = ("yh", "z"), ("x", "yl", "core")
    return jax.shard_map(
        step,
        mesh=torus,
        in_specs=(P(col, row), P(row, col), P(row, col, None, None)),
        out_specs=(P(row, col, None, None), P(row, col)),
        check_vma=False,
    )
```

```python
import jax
import jax.numpy as jnp
from jax import lax
from jax.experimental import pallas as pl
from jax.experimental.pallas import tpu as pltpu
from jax.sharding import Mesh
from jax.sharding import PartitionSpec as P


DAMP = 10.0 ** (-3)
DECAY = 0.9
EPS = 1e-06
F32 = jnp.float32
BF16 = jnp.bfloat16
TILE = 256
SIZES = (640, 384)


VMEM = pl.BlockSpec(memory_space=pltpu.VMEM)
SMEM = pl.BlockSpec(memory_space=pltpu.SMEM)


def shift(value, axis, step):
    count = lax.axis_size(axis)
    return lax.ppermute(value, axis, [(k, (k + step) % count) for k in range(count)])


def aligned(start, size):
    return pl.ds(pl.multiple_of(start, size), size)


def split(value):
    high = value.astype(BF16)
    return high, (value - high.astype(F32)).astype(BF16)


def put_left(left, rows, cols, value):
    n = left.shape[0]
    high, low = split(value)
    left[rows, cols] = high
    left[rows, n + cols.start : n + cols.stop] = high
    left[rows, 2 * n + cols.start : 2 * n + cols.stop] = low


def put_right(right, rows, cols, value):
    n = right.shape[1]
    high, low = split(value)
    right[rows, cols] = high
    right[n + rows.start : n + rows.stop, cols] = low
    right[2 * n + rows.start : 2 * n + rows.stop, cols] = high


def put_symmetric(put, target, j, upper):
    start = j * TILE
    cols = slice(start, start + TILE)
    put(target, slice(0, start + TILE), cols, upper)
    for i in range(j):
        part = slice(i * TILE, (i + 1) * TILE)
        put(target, cols, part, upper[part, :].T)


def symmetric_product(left, right, emit):
    for j in range(right.shape[1] // TILE):
        start = j * TILE
        upper = jnp.dot(
            left[: start + TILE, :], right[:, start : start + TILE], preferred_element_type=F32
        )
        emit(j, upper)


def square_kernel(where, own, other, factor, square, stat, left, right):
    n = stat.shape[0]
    half = n // 2
    h = where[0]
    mine, his = aligned(h * half, half), aligned((1 - h) * half, half)
    stat[mine, :] = own[...]
    step, start, width = other.shape[0], 0, half
    for k in range(half // other.shape[0]):
        rows = aligned((1 - h) * half + k * step, step)
        stat[rows, aligned((1 - h) * half + k * step, step)] = other[:, start : start + step]
        for j in range(1, width // step):
            cols = aligned((1 - h) * half + (k + j) * step, step)
            block = other[:, start + j * step : start + (j + 1) * step]
            stat[rows, cols] = block
            stat[cols, rows] = block.T
        start, width = start + width, width - step
    stat[his, mine] = own[:, his].T

    row = lax.broadcasted_iota(jnp.int32, (TILE, TILE), 0)
    eye = row == lax.broadcasted_iota(jnp.int32, (TILE, TILE), 1)

    def sums(k, carry):
        trace, most = carry
        cols = aligned(k * TILE, TILE)
        trace += jnp.sum(jnp.where(eye, stat[cols, cols], 0.0))
        return trace, jnp.maximum(most, jnp.max(jnp.sum(jnp.abs(stat[:, cols]), axis=0)))

    trace, most = lax.fori_loop(0, n // TILE, sums, (F32(0.0), F32(0.0)))
    damping = DAMP * trace / n
    inverse = 1.0 / (most + damping)
    for i in range(n // TILE):
        rows = slice(i * TILE, (i + 1) * TILE)
        for j in range(n // TILE):
            cols = slice(j * TILE, (j + 1) * TILE)
            value = -stat[rows, cols] * inverse
            if i == j:
                value = jnp.where(eye, (1.25 - damping * inverse) + value, value)
            factor[rows, cols] = value
            put_left(left, rows, cols, value)
            put_right(right, rows, cols, value)

    def squared(j, upper):
        end = (j + 1) * TILE
        square[:end, j * TILE : end] = upper

    symmetric_product(left, right, squared)


def root_kernel(factor, square, root, left, right, left2, right2):
    for j in range(factor.shape[0] // TILE):
        end = (j + 1) * TILE
        upper = square[:end, j * TILE : end]
        put_symmetric(put_left, left2, j, upper)
        put_symmetric(put_right, right2, j, upper)

    def fourth(j, upper):
        end = (j + 1) * TILE
        cols = slice(j * TILE, end)
        put_symmetric(put_left, left, j, upper)
        put_symmetric(put_right, right, j, 5.0 * factor[:end, cols] - 4.0 * square[:end, cols])

    symmetric_product(left2, right2, fourth)

    def last(j, upper):
        end = (j + 1) * TILE
        cols = slice(j * TILE, end)
        value = 1.25 * factor[:end, cols] - 0.25 * upper
        root[:end, cols] = value.astype(BF16)
        for i in range(j):
            part = slice(i * TILE, (i + 1) * TILE)
            root[cols, part] = value[part, :].T.astype(BF16)

    symmetric_product(left, right, last)


def times(left, right):
    return jnp.dot(left, right, preferred_element_type=F32)


LAST = 6


def add_own(total, j, own, grads, part):
    half = grads.shape[1] // 2
    if j == 2:
        total[:, part] += times(grads[:, :half], own[3][...]) + times(grads[:, half:], own[4][...])
    else:
        total[:, part] += times(grads, own[(0, 1, 3, 2)[j]][...])


def own_kernel(slot, *refs):
    own, grads, (total, right, stack) = refs[:5], refs[5:12], refs[12:]
    tokens, width = right.shape[2], right.shape[1] // 2
    for k, piece in zip([k for k in range(8) if k != LAST], grads):
        stack[slot[k], :width, :] = piece[:tokens, :].T
        stack[slot[k], width:, :] = piece[tokens:, :].T
    right[...] = stack[4:]
    total[...] = jnp.zeros(total.shape, F32)
    for j in range(4):
        @pl.when(slot[LAST] != j)
        def _(j=j):
            add_own(total, j, own, stack[j], slice(None))


def partner_kernel(m):
    start = sum(SIZES[:m])

    def add(slot, own, pieces, right, before, late, total):
        value = before[:, start : start + total.shape[1]]
        for k in range(4):
            value += times(right[k], pieces[k][...])
        total[...] = value
        part = pl.ds(start, total.shape[1])
        views = [piece.at[:, part] for piece in own]
        for j in range(4):
            @pl.when(slot[LAST] == j)
            def _(j=j):
                add_own(total, j, views, late[...], slice(None))

    def first(slot, *refs):
        own, pieces, (last, right, before, total, full, late) = refs[:5], refs[5:9], refs[9:]
        tokens, width = right.shape[2], right.shape[1] // 2
        late[:width, :] = last[:tokens, :].T
        late[width:, :] = last[tokens:, :].T
        full[...] = right[...]

        @pl.when(slot[LAST] >= 4)
        def _():
            full[jnp.maximum(slot[LAST] - 4, 0)] = late[...]

        add(slot, own, pieces, full, before, late, total)

    def second(slot, *refs):
        own, pieces, (right, before, late, total) = refs[:5], refs[5:9], refs[9:]
        add(slot, own, pieces, right, before, late, total)

    return second if m else first


def gram_kernel(where, own, *refs):
    tiles, (renewed, block) = refs[:8], refs[8:]
    n = block.shape[0]
    width = tiles[0].shape[0]
    half = n // 2
    h, s = where[0], where[1]
    for dh in range(2):
        for ds in range(2):
            cols = aligned((2 * (h + dh - 2 * h * dh) + (s + ds - 2 * s * ds)) * width, width)
            block[cols, : SIZES[0]] = tiles[2 * dh + ds][...]
            block[cols, SIZES[0] :] = tiles[4 + 2 * dh + ds][...]
    rows = aligned(h * half, half)

    def renew(gram):
        renewed[...] = DECAY * own[...] + ((1.0 - DECAY) / n) * gram

    @pl.when(s == 0)
    def _():
        renew(lax.dot_general(
            block[:, rows], block[...], (((0,), (0,)), ((), ())), preferred_element_type=F32))

    @pl.when(s == 1)
    def _():
        renew(lax.dot_general(
            block[rows, :], block[...], (((1,), (1,)), ((), ())), preferred_element_type=F32))


def update_kernel(where, block, mine, other, update, cond):
    n, width = update.shape
    h, s = where[0], where[1]
    tile = aligned((2 * h + s) * width, width)

    def condition(left, right):
        product = times(right[tile, :], block[...]).astype(BF16)
        cond[...] = times(product, left[...])

    @pl.when(s == 0)
    def _():
        condition(mine, other)

    @pl.when(s == 1)
    def _():
        condition(other, mine)

    values = block[tile, :].astype(F32)
    conditioned = cond[...]
    count = n * width
    power = jnp.sum(values * values) / count
    base = jnp.sum(conditioned * conditioned) / count + EPS
    update[...] = (conditioned * jnp.sqrt(power / base)).astype(BF16).T


def resident(value):
    return pltpu.with_memory_space_constraint(value, pltpu.VMEM)


def call(kernel, out, args, in_specs, out_specs, scratch, flops, limit):
    return pl.pallas_call(
        kernel,
        out_shape=out,
        in_specs=in_specs,
        out_specs=out_specs,
        scratch_shapes=scratch,
        cost_estimate=pl.CostEstimate(flops=flops, transcendentals=0, bytes_accessed=2**23),
        compiler_params=pltpu.CompilerParams(vmem_limit_bytes=limit * 2**20),
    )(*[arg if spec is SMEM else resident(arg) for arg, spec in zip(args, in_specs)])


def root_of(where, own, other):
    n = own.shape[1]
    wide = pltpu.VMEM((n, n), F32)
    pair = [pltpu.VMEM((n, 3 * n), BF16), pltpu.VMEM((3 * n, n), BF16)]
    factor, square = call(
        square_kernel, (wide, wide), (where, own, other),
        [SMEM, VMEM, VMEM], (VMEM, VMEM), [wide] + pair, 4 * n**3, 20,
    )
    return call(
        root_kernel, pltpu.VMEM((n, n), BF16), (factor, square),
        [VMEM, VMEM], VMEM, pair + pair, 8 * n**3, 28,
    )


def own_gradient(slot, own, grads):
    tokens, rows = own[0].shape
    width = 2 * grads[0].shape[1]
    return call(
        own_kernel,
        (pltpu.VMEM((width, rows), F32), pltpu.VMEM((4, width, tokens), BF16)),
        (slot, *own, *grads), [SMEM] + [VMEM] * 12, (VMEM, VMEM),
        [pltpu.VMEM((8, width, tokens), BF16)], 8 * tokens * rows * width, 14,
    )


def whole_gradient(m, slot, own, partner, right, before, last):
    width, tokens = right.shape[1:]
    out = [pltpu.VMEM((width, SIZES[m]), F32)]
    args = (slot, *own, *partner, right, before, last)
    if m == 0:
        out += [pltpu.VMEM(right.shape, BF16), pltpu.VMEM((width, tokens), BF16)]
        args = (slot, *own, *partner, last, right, before)
    return call(
        partner_kernel(m), tuple(out), args, [SMEM] + [VMEM] * 12,
        (VMEM,) * len(out), [], 8 * tokens * SIZES[m] * width, 10,
    )


def finish(where, own, mine, other, tiles):
    n = mine.shape[0]
    half, width = n // 2, tiles[0].shape[0]
    renewed, block = call(
        gram_kernel, (jax.ShapeDtypeStruct((half, n), F32), pltpu.VMEM((n, n), BF16)),
        (where, own, *tiles), [SMEM] + [VMEM] * (1 + len(tiles)), (VMEM, VMEM), [], 2 * n**3, 12,
    )
    update = call(
        update_kernel, jax.ShapeDtypeStruct((n, width), BF16),
        (where, block, mine, other), [SMEM] + [VMEM] * 3, VMEM, [pltpu.VMEM((width, n), F32)],
        2 * n**3, 12,
    )
    return renewed, update


def step(activations, out_grads, statistics):
    own = statistics[0, 0]
    half, _ = own.shape
    width = out_grads.shape[1]
    x, z, yh = lax.axis_index("x"), lax.axis_index("z"), lax.axis_index("yh")
    h, s = lax.axis_index("yl"), lax.axis_index("core")
    where = jnp.stack([h, s]).astype(jnp.int32)

    cut = activations.shape[0] // 2
    below, above = shift(activations, "x", 1), shift(activations, "x", -1)
    far = [shift(below[:cut], "x", 1), shift(above[cut:], "x", -1)]
    mine = [activations, above, below] + far
    partner = []
    for m, size in enumerate(SIZES):
        start = sum(SIZES[:m])
        across = shift(activations[:, start : start + size], "yl", 1)
        below, above = shift(across, "x", 1), shift(across, "x", -1)
        last = shift(below, "x", 1) if m == 0 else shift(above, "x", -1)
        partner.append([across, above, last, below])

    tokens = out_grads.shape[0] // 2
    keep = lax.dynamic_slice_in_dim(out_grads, s * tokens, tokens, 0)
    give = lax.dynamic_slice_in_dim(out_grads, (1 - s) * tokens, tokens, 0)
    pair = jnp.concatenate([keep, shift(give, "core", 1)], 0)
    across = shift(pair, "yh", 1)
    below, above = shift(pair, "z", 1), shift(pair, "z", -1)
    grads = [pair, above, shift(below, "z", 1), below]
    below, above = shift(across, "z", 1), shift(across, "z", -1)
    grads += [across, above, shift(above, "z", -1), below]
    slot = []
    for dy in range(2):
        for dz in range(4):
            chunk = 4 * ((yh + dy) % 2) + (z + dz) % 4
            slot.append(4 * ((chunk + h) % 2) + (chunk // 2 - x) % 4)
    slot = jnp.stack(slot).astype(jnp.int32)

    quadrant = lax.dynamic_slice_in_dim(own, h * half, half, 1)
    cut = half // 4
    packed = [quadrant[k : k + cut, k:] for k in range(0, half, cut)]
    packed = jnp.concatenate(packed, 1)
    root = root_of(where, own, shift(packed, "yl", 1))
    other = shift(root, "core", 1)

    last = grads.pop(LAST)
    part, right = own_gradient(slot, mine, grads)
    tiles = []
    for m in range(2):
        if m == 0:
            total, right, last = whole_gradient(m, slot, mine, partner[m], right, part, last)
        else:
            (total,) = whole_gradient(m, slot, mine, partner[m], right, part, last)
        given = shift(total, "core", 1)
        tile = (total[:width] + given[width:]).astype(BF16)
        beside = (total[width:] + given[:width]).astype(BF16)
        across = shift(tile, "yl", 1)
        tiles += [tile, beside, across, shift(across, "core", 1)]

    renewed, update = finish(where, own, root, other, tiles)
    return renewed[None, None], update


def solution(mesh):
    torus = Mesh(mesh.devices.reshape(2, 4, 4, 2, 2), ("yh", "z", "x", "yl", "core"))
    row, col = ("yh", "z"), ("x", "yl", "core")
    return jax.shard_map(
        step,
        mesh=torus,
        in_specs=(P(col, row), P(row, col), P(row, col, None, None)),
        out_specs=(P(row, col, None, None), P(row, col)),
        check_vma=False,
    )
```
